256 devices in a mesh: seq: 256 (over x, z, y, core).
Axes of the slice: x: 4, y: 4, z: 8, core: 2. Of those that a mesh axis runs over, the one named last changes fastest.
Arguments:
- queries: bfloat16 [65536, 8, 128], P('seq'), may hold values from -6 to 6
- key_rows: bfloat16 [65536, 4, 128], P('seq'), may hold values from -6 to 6
- value_rows: bfloat16 [65536, 4, 128], P('seq'), may hold values from -6 to 6
- attn_output: bfloat16 [65536, 8, 128], P('seq'), may hold values from -6 to 6
- grad_output: bfloat16 [65536, 8, 128], P('seq'), may hold values from -144 to 144
- log_norm: float32 [8, 65536], P(None, 'seq'), may hold values from 6.5 to 8
Outputs:
- grad_queries: bfloat16 [65536, 8, 128], P('seq')
- grad_keys: bfloat16 [65536, 4, 128], P('seq')
- grad_values: bfloat16 [65536, 4, 128], P('seq')
The draws below stay inside these ranges and needn't reach their ends.
All inputs are finite; a program needn't handle non-finite values.
Results may differ from the reference program's by a relative error of at most 0.0057.
Values may be sent and summed in bfloat16 or wider, within the bound.
A program may use at most 64 MiB of HBM per device.

```python
import jax
import jax.numpy as jnp
from jax import lax

HD = 128
QH = 8
KVH = 4
W = 1024
TOK_DEV = 256
TOKENS = 65536


def levels(key, shape, split, low, largest):
    loudness = 1.0
    for position, parts in split:
        draws = jax.random.uniform(jax.random.fold_in(jax.random.fold_in(key, 6), position), (parts,), jnp.float32, low / len(split), largest / len(split))
        loudness = loudness * jnp.repeat(jnp.exp(draws), shape[position] // parts).reshape((-1,) + (1,) * (len(shape) - 1 - position))
    return loudness


def gaussian(rng, shape, width, reach, pieces=(), kind=jnp.bfloat16):
    entries = width * jax.random.normal(rng, shape, jnp.float32)
    if pieces:
        entries = entries * levels(rng, shape, pieces, -0.22, 0.18)
    return jnp.clip(entries, -reach, reach).astype(kind)


def setup_inputs(seed: int = 0) -> dict:
    key_of = jax.random.split(jax.random.key(seed), 7)
    queries = gaussian(key_of[0], (TOKENS, QH, HD), 1.0, 6.0, ((0, 256),))
    key_rows = gaussian(key_of[1], (TOKENS, KVH, HD), 1.0, 6.0, ((0, 256),))
    value_rows = gaussian(key_of[2], (TOKENS, KVH, HD), 1.0, 6.0, ((0, 256),))
    attn_output = gaussian(key_of[3], (TOKENS, QH, HD), 1.0, 6.0, ((0, 256),))
    grad_output = gaussian(key_of[4], (TOKENS, QH, HD), 24.0, 144.0, ((0, 256),))
    log_norm = jnp.clip(6.5 + 1.5 * jax.random.uniform(key_of[5], (QH, TOKENS), jnp.float32) ** levels(key_of[5], (QH, TOKENS), ((1, 256),), -0.2, 0.2), 6.5, 8.0)
    return dict(queries=queries, key_rows=key_rows, value_rows=value_rows, attn_output=attn_output, grad_output=grad_output, log_norm=log_norm)


query_scale = 168.0 ** -0.5


def band_mask(query_pos, key_pos, seq_rows):
    offset = query_pos[:, None] - key_pos[None, :]
    inside = (offset >= 0) & (offset < W)
    return inside & (key_pos >= 0)[None, :] & (query_pos < seq_rows)[:, None]


def band_grads(queries, grad_output, log_norm, delta_rows, key_rows, value_rows, allowed):
    row_count, head_count, head_size = queries.shape
    group_count = key_rows.shape[1]
    share = head_count // group_count
    query_group = queries.reshape(row_count, group_count, share, head_size).astype(jnp.float32)
    grad_group = grad_output.reshape(row_count, group_count, share, head_size).astype(jnp.float32)
    key_float = key_rows.astype(jnp.float32)
    value_float = value_rows.astype(jnp.float32)
    scores = jnp.einsum("qkgd,lkd->kgql", query_group, key_float) * query_scale
    norm_part = log_norm.reshape(group_count, share, row_count)[..., None]
    delta_part = delta_rows.reshape(group_count, share, row_count)[..., None]
    probs = jnp.where(allowed[None, None], jnp.exp(scores - norm_part), 0.0)
    probs_low = lax.optimization_barrier(probs.astype(jnp.bfloat16)).astype(jnp.float32)
    grad_v = jnp.einsum("kgql,qkgd->lkd", probs_low, grad_group)
    dprobs = jnp.einsum("qkgd,lkd->kgql", grad_group, value_float)
    dscores = lax.optimization_barrier((probs * (dprobs - delta_part)).astype(jnp.bfloat16)).astype(jnp.float32)
    grad_q = jnp.einsum("kgql,lkd->qkgd", dscores, key_float) * query_scale
    grad_k = jnp.einsum("kgql,qkgd->lkd", dscores, query_group) * query_scale
    return grad_q.reshape(row_count, head_count, head_size), grad_k, grad_v


def reference(queries, key_rows, value_rows, attn_output, grad_output, log_norm):
    total_rows = queries.shape[0]
    row_block = min(TOK_DEV, 128)
    hop_count = W // TOK_DEV
    front = jnp.zeros((W,) + key_rows.shape[1:], key_rows.dtype)
    padded_keys = jnp.concatenate([front, key_rows], 0)
    padded_values = jnp.concatenate([front, value_rows], 0)
    delta_rows = jnp.sum(grad_output.astype(jnp.float32) * attn_output.astype(jnp.float32), axis=-1).T
    distances = jnp.arange(hop_count + 1, dtype=jnp.int32)

    def visit(carry, block_index):
        total_k, total_v = carry
        start = (block_index * row_block).astype(jnp.int32)
        span = W + row_block
        query_pos = start + jnp.arange(row_block, dtype=jnp.int32)
        key_pos = start - W + jnp.arange(span, dtype=jnp.int32)
        allowed = band_mask(query_pos, key_pos, total_rows)
        grad_q, grad_k, grad_v = band_grads(
            lax.dynamic_slice_in_dim(queries, start, row_block, 0),
            lax.dynamic_slice_in_dim(grad_output, start, row_block, 0),
            lax.dynamic_slice_in_dim(log_norm, start, row_block, 1),
            lax.dynamic_slice_in_dim(delta_rows, start, row_block, 1),
            lax.dynamic_slice_in_dim(padded_keys, start, span, 0),
            lax.dynamic_slice_in_dim(padded_values, start, span, 0),
            allowed)
        query_dev = start // TOK_DEV
        key_dev = jnp.floor_divide(key_pos, TOK_DEV)
        apart = jnp.clip(query_dev - key_dev, 0, hop_count).astype(jnp.int32)
        picks = (apart[None, :] == distances[:, None]).astype(jnp.float32)[:, :, None, None]
        total_k = lax.dynamic_update_slice_in_dim(total_k, lax.dynamic_slice_in_dim(total_k, start, span, 1) + picks * grad_k[None], start, 1)
        total_v = lax.dynamic_update_slice_in_dim(total_v, lax.dynamic_slice_in_dim(total_v, start, span, 1) + picks * grad_v[None], start, 1)
        return (total_k, total_v), grad_q

    zeros_init = jnp.zeros((hop_count + 1, W + total_rows) + key_rows.shape[1:], jnp.float32)
    (total_k, total_v), grad_blocks = lax.scan(visit, (zeros_init, zeros_init), jnp.arange(total_rows // row_block, dtype=jnp.int32))
    grad_queries = grad_blocks.reshape(queries.shape).astype(jnp.bfloat16)
    far_k = lax.optimization_barrier(total_k[1:].astype(jnp.bfloat16)).astype(jnp.float32)
    far_v = lax.optimization_barrier(total_v[1:].astype(jnp.bfloat16)).astype(jnp.float32)
    own_k = total_k[0] + jnp.sum(far_k, axis=0)
    own_v = total_v[0] + jnp.sum(far_v, axis=0)
    return grad_queries, own_k[W:].astype(jnp.bfloat16), own_v[W:].astype(jnp.bfloat16)
```

```python
import functools
import math

import jax
import jax.numpy as jnp
from jax import lax
from jax.experimental import pallas as pl
from jax.experimental.pallas import tpu as pltpu
from jax.sharding import PartitionSpec as P

MESH = pl.DeviceIdType.MESH
BF = jnp.bfloat16
F32 = jnp.float32
SCALE = 168.0 ** (-0.5)
LOG2E = math.log2(math.e)
T = 256
HD = 128
NC = 4
TC = T // NC
NU = 2 * NC
FAR = 1e30


def dot_nt(a, b):
    return lax.dot_general(a, b, (((1,), (1,)), ((), ())), preferred_element_type=F32)


def dot_nn(a, b):
    return lax.dot_general(a, b, (((1,), (0,)), ((), ())), preferred_element_type=F32)


def dot_tn(a, b):
    return lax.dot_general(a, b, (((0,), (0,)), ((), ())), preferred_element_type=F32)


def kernel(
    n,
    q_hbm, k_hbm, v_hbm, o_hbm, g_hbm, lse_hbm,
    gq_out, gk_out, gv_out,
    kraw, kv_x, qb, gb, qx, gx, ob, lse_s, st, stx, kd, kf,
    acc_h, acc_l, acc_z, dq_t, dqs, g2s, g2r, g1s, g1r, g0r, fi, fo,
    kv_ld, in_ld,
    o_send, o_recv, r_send, r_recv, g2_send, g2_recv, g1_send, g1_recv,
    x_send, x_recv, dq_send, dq_recv, out_sem,
):
    me = lax.axis_index("seq")
    k = lax.rem(me, 2)
    oth = 1 - k
    chip = lax.div(me, 2)
    up = lax.rem(me - k + 2, n)
    down = lax.rem(me - k + n - 2, n)
    partner = me - k + oth

    def remote(src, dst, ssem, rsem, dev):
        return pltpu.make_async_remote_copy(
            src_ref=src, dst_ref=dst, send_sem=ssem, recv_sem=rsem,
            device_id=(dev,), device_id_type=MESH,
        )

    def par(u):
        return k if u % 2 == 0 else oth

    kv_loads = []
    for m in range(NC):
        rows = pl.ds(m * TC, TC)
        for i, (dst, pair) in enumerate(((kraw.at[4 + k, m], k), (kv_x.at[m], oth))):
            for e, src in enumerate((k_hbm, v_hbm)):
                kv_loads.append(
                    pltpu.make_async_copy(src.at[rows, pair], dst.at[e], kv_ld.at[m, i, e])
                )
    for c in kv_loads:
        c.start()
    in_loads = []
    s = 0
    for src, near, far in ((q_hbm, qb.at[k], qx), (g_hbm, gb.at[k], gx), (o_hbm, ob.at[0], ob.at[1])):
        for dst, base in ((near, k), (far, oth)):
            for j in range(2):
                in_loads.append(
                    pltpu.make_async_copy(src.at[:, 2 * base + j], dst.at[j], in_ld.at[s])
                )
                s += 1
    in_loads.append(pltpu.make_async_copy(lse_hbm, lse_s, in_ld.at[s]))
    for c in in_loads:
        c.start()

    bar = pltpu.get_barrier_semaphore()
    for dev in (up, up + 1, down, down + 1, partner):
        pl.semaphore_signal(bar, inc=1, device_id=(dev,), device_id_type=MESH)
    pl.semaphore_wait(bar, 5)

    def own_copy(u):
        m = u // 2
        src = kraw.at[4 + k, m] if u % 2 == 0 else kv_x.at[m]
        dev = up + par(u)
        return remote(src, kraw.at[2 + k, m], o_send.at[u], o_recv.at[k, m], dev)

    def own_arrival(u):
        m = u // 2
        x = par(u)
        return remote(kraw.at[2 + x, m], kraw.at[2 + x, m], o_send.at[u], o_recv.at[x, m], up)

    def relay_copy(u):
        m = u // 2
        x = par(u)
        return remote(kraw.at[2 + x, m], kraw.at[x, m], r_send.at[u], r_recv.at[x, m], up + k)

    def g2_copy(u):
        m = u // 2
        x = par(u)
        return remote(g2s.at[x, m], g2r.at[x, m], g2_send.at[u], g2_recv.at[x, m], down + k)

    def g1_copy(u):
        m = u // 2
        x = par(u)
        return remote(g1s.at[x, m], g1r.at[k, m], g1_send.at[u], g1_recv.at[k, m], down + x)

    def g1_arrival(u):
        m = u // 2
        p = par(u)
        return remote(g1s.at[p, m], g1r.at[p, m], g1_send.at[u], g1_recv.at[p, m], down)

    x_kv = remote(kv_x, kraw.at[4 + k], x_send.at[0], x_recv.at[0], partner)
    x_q = remote(qx, qb.at[k], x_send.at[1], x_recv.at[1], partner)
    x_g = remote(gx, gb.at[k], x_send.at[2], x_recv.at[2], partner)
    x_st = remote(stx, st.at[k], x_send.at[3], x_recv.at[3], partner)
    g0_copy = remote(acc_l.at[oth], g0r, x_send.at[4], x_recv.at[4], partner)

    def kv_wait(m, i):
        for e in range(2):
            kv_loads[(m * 2 + i) * 2 + e].wait()

    kv_wait(0, 0)
    own_copy(0).start()
    kv_wait(0, 1)
    own_copy(1).start()
    for m in range(1, NC):
        kv_wait(m, 0)
        kv_wait(m, 1)
    x_kv.start()
    for i in (2, 3):
        in_loads[i].wait()
    x_q.start()
    for i in (6, 7):
        in_loads[i].wait()
    x_g.start()
    for i in (0, 1, 4, 5, 8, 9, 10, 11, 12):
        in_loads[i].wait()

    def flat(val):
        return val.reshape(val.shape[0] * 2, HD)

    lse = lse_s[...] * LOG2E
    hi = lse.astype(BF)
    rest = lse - hi.astype(F32)
    mid = rest.astype(BF)
    low = (rest - mid.astype(F32)).astype(BF)
    parts = jnp.concatenate([hi.astype(F32), mid.astype(F32), low.astype(F32), jnp.zeros_like(lse)], 0).astype(BF)
    row = lax.broadcasted_iota(jnp.int32, (T, 2 * T), 0)
    col = lax.broadcasted_iota(jnp.int32, (T, 2 * T), 1)
    wide = []
    for e in range(2):
        place = jnp.where(col == 2 * row + e, 1.0, 0.0).astype(BF)
        r = dot_nn(parts, place)
        wide.append(r[0:8] + r[8:16] + r[16:24])
    lse_w = [wide[0][2 * i : 2 * i + 1] + wide[1][2 * i + 1 : 2 * i + 2] for i in range(4)]
    ones = jnp.ones((8, HD), BF)

    def delta_of(a, b):
        prod = a.astype(F32) * b.astype(F32)
        top = prod.astype(BF)
        left = (prod - top.astype(F32)).astype(BF)
        return (dot_nt(ones, top) + dot_nt(ones, left))[0:1]

    no_1 = jnp.where(chip < 1, FAR, 0.0).astype(F32)
    no_2 = jnp.where(chip < 2, FAR, 0.0).astype(F32)
    for j in range(2):
        for which in range(2):
            if which == 0:
                dst, dl = st.at[k, j], delta_of(flat(gb[k, j]), flat(ob[0, j]))
            else:
                dst, dl = stx.at[j], delta_of(flat(gx[j]), flat(ob[1, j]))
            if which == 0:
                lw = jnp.where(k == 0, lse_w[j], lse_w[2 + j])
            else:
                lw = jnp.where(k == 0, lse_w[2 + j], lse_w[j])
            dst[0:1, :] = lw
            dst[1:2, :] = dl
            dst[2:3, :] = lw + no_1
            dst[3:4, :] = lw + no_2
            dst[4:8, :] = jnp.zeros((4, 2 * T), F32)
    x_st.start()
    dq_t[...] = jnp.zeros_like(dq_t)

    def split(src, slot):
        for e in range(2):
            kf[slot, e] = flat(src[e]).astype(F32)
        for e in range(2):
            for j in range(2):
                kd[slot, e, j] = kf[slot, e, pl.ds(j, TC, stride=2), :].astype(BF)

    def tile(slot, b, j, lo, hi, norm_row, mask):
        kc, vc = kd[slot, 0, j], kd[slot, 1, j]
        q, g = flat(qb[b, j, lo // 2 : hi // 2]), flat(gb[b, j, lo // 2 : hi // 2])
        sc = dot_nt(kc, q)
        p = jnp.exp2(sc * (SCALE * LOG2E) - st[b, j, norm_row : norm_row + 1, lo:hi])
        if mask is not None:
            p = jnp.where(mask, p, 0.0)
        dv = dot_nn(p.astype(BF), g)
        dp = dot_nt(vc, g)
        ds = (p * (dp - st[b, j, 1:2, lo:hi])).astype(BF)
        dk = dot_nn(ds, q)
        dq_t[b, j, :, lo:hi] += dot_tn(kc, ds)
        return dk, dv

    def tri(m, lo, hi, upper):
        key = m * TC + lax.broadcasted_iota(jnp.int32, (TC, hi - lo), 0)
        tok = (lo + lax.broadcasted_iota(jnp.int32, (TC, hi - lo), 1)) // 2
        return key > tok if upper else tok >= key

    def local_causal(x):
        for m in range(NC):
            split(kraw.at[4 + x, m], 0)
            lo = 2 * m * TC
            for j in range(2):
                dk, dv = tile(0, x, j, lo, 2 * T, 0, tri(m, lo, 2 * T, False))
                acc_l[x, 0, j, pl.ds(m * TC, TC), :] = dk
                acc_l[x, 1, j, pl.ds(m * TC, TC), :] = dv

    def local_full():
        for m in range(NC):
            split(kraw.at[4, m], 0)
            for j in range(2):
                dk, dv = tile(0, 1, j, 0, 2 * T, 0, None)
                acc_l[0, 0, j, pl.ds(m * TC, TC), :] += dk
                acc_l[0, 1, j, pl.ds(m * TC, TC), :] += dv

    def near_unit(u):
        m, x = u // 2, par(u)
        split(kraw.at[2 + x, m], 1)
        for j in range(2):
            dk0, dv0 = tile(1, 0, j, 0, 2 * T, 2, None)
            dk1, dv1 = tile(1, 1, j, 0, 2 * T, 2, None)
            acc_h[x, m, 0, j] = dk0 + dk1
            acc_h[x, m, 1, j] = dv0 + dv1

    def far_unit(u):
        m, x = u // 2, par(u)
        split(kraw.at[x, m], 2)
        hi = 2 * (m + 1) * TC
        for j in range(2):
            dk, dv = tile(2, x, j, 0, hi, 3, tri(m, 0, hi, True))
            acc_z[0, j] = dk
            acc_z[1, j] = dv

        @pl.when(x == 1)
        def _():
            for j in range(2):
                dk, dv = tile(2, 0, j, 0, 2 * T, 3, None)
                acc_z[0, j] += dk
                acc_z[1, j] += dv

        g2s[x, m] = acc_z[...].astype(BF)

    def near_finish(u):
        m, x = u // 2, par(u)
        g1s[x, m] = (acc_h[x, m] + g2r[x, m].astype(F32)).astype(BF)

    outs = []

    def final_unit(u):
        m, p = u // 2, par(u)
        rows = pl.ds(m * TC, TC)
        for e in range(2):
            for j in range(2):
                mine = acc_l[k, e, j, rows, :] if u % 2 == 0 else g0r[e, j, rows, :]
                val = mine + g1r[p, m, e, j].astype(F32)
                if e == 0:
                    val = val * SCALE
                fi[e, pl.ds(j, TC, stride=2), :] = val
            fo[u, e] = fi[e].astype(BF).reshape(TC, 2, HD)
            dst = (gk_out, gv_out)[e]
            c = pltpu.make_async_copy(fo.at[u, e], dst.at[rows, p], out_sem.at[2 * u + e])
            c.start()
            outs.append(c)

    def arrive(u):
        own_arrival(u).wait_recv()
        relay_copy(u).start()
        if u + 2 < NU:
            own_copy(u + 2).start()

    def far_step(u):
        relay_copy(u).wait_recv()
        far_unit(u)
        g2_copy(u).start()

    def near_step(u):
        g2_copy(u).wait_recv()
        near_finish(u)
        g1_copy(u).start()

    def final_step(u):
        g1_arrival(u).wait_recv()
        final_unit(u)

    local_causal(k)
    arrive(0)
    x_kv.wait_recv()
    x_q.wait_recv()
    x_g.wait_recv()
    x_st.wait_recv()
    local_causal(oth)
    arrive(1)
    local_full()
    g0_copy.start()
    near_unit(0)
    near_unit(1)
    far_step(0)
    for u in range(2, NU):
        arrive(u)
        near_unit(u)
        far_step(u - 1)
        near_step(u - 2)
        if u == 4:
            g0_copy.wait_recv()
        if u >= 4:
            final_step(u - 4)
    far_step(NU - 1)

    dq_copies = []
    for j in range(2):
        for b, dst_dev in ((oth, partner), (k, None)):
            dqs[b, j] = (dq_t[b, j].T * SCALE).astype(BF).reshape(T, 2, HD)
            if dst_dev is None:
                c = pltpu.make_async_copy(dqs.at[b, j], gq_out.at[:, 2 * k + j], out_sem.at[2 * NU + j])
                c.start()
                outs.append(c)
            else:
                c = remote(dqs.at[b, j], gq_out.at[:, 2 * k + j], dq_send.at[j], dq_recv.at[j], partner)
                c.start()
                dq_copies.append(c)

    near_step(NU - 2)
    final_step(NU - 4)
    final_step(NU - 3)
    near_step(NU - 1)
    final_step(NU - 2)
    final_step(NU - 1)

    for u in range(NU):
        own_copy(u).wait_send()
        relay_copy(u).wait_send()
        g2_copy(u).wait_send()
        g1_copy(u).wait_send()
    for c in (x_kv, x_q, x_g, x_st, g0_copy):
        c.wait_send()
    for c in dq_copies:
        c.wait()
    for c in outs:
        c.wait()


def shards(n, queries, key_rows, value_rows, attn_output, grad_output, log_norm):
    heads4 = (T, 4, 2, HD)
    heads2 = (T, 2, 2, HD)
    anym = pl.BlockSpec(memory_space=pl.ANY)
    dma = pltpu.SemaphoreType.DMA
    vm = pltpu.VMEM
    pair = (T, 2, HD)
    scratch = [
        vm((6, NC, 2, TC, 2, HD), BF),
        vm((NC, 2, TC, 2, HD), BF),
        vm((2, 2) + pair, BF),
        vm((2, 2) + pair, BF),
        vm((2,) + pair, BF),
        vm((2,) + pair, BF),
        vm((2, 2) + pair, BF),
        vm((8, T), F32),
        vm((2, 2, 8, 2 * T), F32),
        vm((2, 8, 2 * T), F32),
        vm((3, 2, 2, TC, HD), BF),
        vm((3, 2, 2 * TC, HD), F32),
        vm((2, NC, 2, 2, TC, HD), F32),
        vm((2, 2, 2, T, HD), F32),
        vm((2, 2, TC, HD), F32),
        vm((2, 2, HD, 2 * T), F32),
        vm((2, 2) + pair, BF),
        vm((2, NC, 2, 2, TC, HD), BF),
        vm((2, NC, 2, 2, TC, HD), BF),
        vm((2, NC, 2, 2, TC, HD), BF),
        vm((2, NC, 2, 2, TC, HD), BF),
        vm((2, 2, T, HD), F32),
        vm((2, 2 * TC, HD), F32),
        vm((NU, 2, TC, 2, HD), BF),
        dma((NC, 2, 2)),
        dma((13,)),
        dma((NU,)), dma((2, NC)),
        dma((NU,)), dma((2, NC)),
        dma((NU,)), dma((2, NC)),
        dma((NU,)), dma((2, NC)),
        dma((5,)), dma((5,)),
        dma((2,)), dma((2,)),
        dma((2 * NU + 2,)),
    ]
    gq, gk, gv = pl.pallas_call(
        functools.partial(kernel, n),
        out_shape=(
            jax.ShapeDtypeStruct(heads4, BF),
            jax.ShapeDtypeStruct(heads2, BF),
            jax.ShapeDtypeStruct(heads2, BF),
        ),
        in_specs=[anym] * 6,
        out_specs=(anym,) * 3,
        scratch_shapes=scratch,
        compiler_params=pltpu.CompilerParams(
            collective_id=0, has_side_effects=True, vmem_limit_bytes=48 << 20
        ),
    )(
        queries.reshape(heads4),
        key_rows.reshape(heads2),
        value_rows.reshape(heads2),
        attn_output.reshape(heads4),
        grad_output.reshape(heads4),
        log_norm,
    )
    return (
        gq.reshape(queries.shape),
        gk.reshape(key_rows.shape),
        gv.reshape(value_rows.shape),
    )


def solution(mesh):
    wide = P("seq", None, None)
    return jax.shard_map(
        functools.partial(shards, mesh.shape["seq"]),
        mesh=mesh,
        in_specs=(wide, wide, wide, wide, wide, P(None, "seq")),
        out_specs=(wide, wide, wide),
        check_vma=False,
    )
```

```python
import functools
import math

import jax
import jax.numpy as jnp
from jax import lax
from jax.experimental import pallas as pl
from jax.experimental.pallas import tpu as pltpu
from jax.sharding import PartitionSpec as P

MESH = pl.DeviceIdType.MESH
BF = jnp.bfloat16
F32 = jnp.float32
SCALE = 168.0 ** (-0.5)
LOG2E = math.log2(math.e)
T = 256
HD = 128
NC = 4
TC = T // NC
NU = 2 * NC
FAR = 1e30
VMEM_KIB = 24 << 10
DIRECT_KV = ()
DIRECT_G = (3,)
PLAN = ('flip0', 'A0', 'A1', 'o2', 'X', 'flip1', 'L0', 'N0', 'F0', 'A2', 'A3', 'o3', 'N1', 'L1', 'S0', 'F1', 'A4', 'A5', 'LF', 'S1', 'F2', 'A6', 'A7', 'N2', 'N3', 'S3', 'F3', 'S2', 'Q', 'Z0', 'Z1', 'Z2', 'Z3', 'D', 'Z4', 'Z5', 'Z6', 'Z7')


def dot_nt(a, b):
    return lax.dot_general(a, b, (((1,), (1,)), ((), ())), preferred_element_type=F32)


def dot_nn(a, b):
    return lax.dot_general(a, b, (((1,), (0,)), ((), ())), preferred_element_type=F32)


def dot_tn(a, b):
    return lax.dot_general(a, b, (((0,), (0,)), ((), ())), preferred_element_type=F32)


def kernel(
    n,
    q_hbm, k_hbm, v_hbm, o_hbm, g_hbm, lse_hbm,
    gq_out, gk_out, gv_out,
    kin, kraw, kv_x, qraw, graw, ob, qf, gf, qt, gt, qx, gx, lse_s, st, stx, kf,
    acc_h, acc_l, dq_t, dqs, g2s, g2r, g1s, g1r, g2d, g0r, fi, fo,
    kv_ld, in_ld,
    o_send, o_recv, r_send, r_recv, g2_send, g2_recv, g1_send, g1_recv, gd_send, gd_recv,
    x_send, x_recv, dq_send, dq_recv, out_sem,
):
    me = lax.axis_index("seq")
    k = lax.rem(me, 2)
    oth = 1 - k
    chip = lax.div(me, 2)
    up = lax.rem(me - k + 2, n)
    down = lax.rem(me - k + n - 2, n)
    up2 = lax.rem(me - k + 4, n)
    down2 = lax.rem(me - k + n - 4, n)
    partner = me - k + oth

    def remote(src, dst, ssem, rsem, dev):
        return pltpu.make_async_remote_copy(
            src_ref=src, dst_ref=dst, send_sem=ssem, recv_sem=rsem,
            device_id=(dev,), device_id_type=MESH,
        )

    def par(u):
        return k if u % 2 == 0 else oth

    kv_loads = []
    for m in range(NC):
        rows = pl.ds(m * TC, TC)
        for i, pair in enumerate((k, oth)):
            for e, src in enumerate((k_hbm, v_hbm)):
                kv_loads.append(
                    pltpu.make_async_copy(src.at[rows, pair], kin.at[i, m, e], kv_ld.at[m, i, e])
                )
    for c in kv_loads:
        c.start()
    in_loads = []
    s = 0
    for src, dst2 in ((q_hbm, qraw), (g_hbm, graw), (o_hbm, ob)):
        for i, base in enumerate((k, oth)):
            for j in range(2):
                in_loads.append(
                    pltpu.make_async_copy(src.at[:, 2 * base + j], dst2.at[i, j], in_ld.at[s])
                )
                s += 1
    in_loads.append(pltpu.make_async_copy(lse_hbm, lse_s, in_ld.at[s]))
    for c in in_loads:
        c.start()

    bar = pltpu.get_barrier_semaphore()
    for dev in (up, up + 1, down, down + 1, up2, up2 + 1, down2, down2 + 1, partner):
        pl.semaphore_signal(bar, inc=1, device_id=(dev,), device_id_type=MESH)
    pl.semaphore_wait(bar, 9)

    def own_copy(u):
        m = u // 2
        src = kraw.at[4 + k, m] if u % 2 == 0 else kv_x.at[m]
        dev = up + par(u)
        return remote(src, kraw.at[2 + k, m], o_send.at[u], o_recv.at[k, m], dev)

    def own_arrival(u):
        m = u // 2
        x = par(u)
        return remote(kraw.at[2 + x, m], kraw.at[2 + x, m], o_send.at[u], o_recv.at[x, m], up)

    def direct_copy(u):
        m = u // 2
        src = kraw.at[4 + k, m] if u % 2 == 0 else kv_x.at[m]
        return remote(src, kraw.at[k, m], r_send.at[u], r_recv.at[k, m], up2 + par(u))

    def relay_copy(u):
        m = u // 2
        x = par(u)
        return remote(kraw.at[2 + x, m], kraw.at[x, m], r_send.at[u], r_recv.at[x, m], up + k)

    def g2_copy(m, j):
        return remote(g2s.at[m, j], g2r.at[m, j], g2_send.at[m, j], g2_recv.at[m, j], down + k)

    def g2d_copy(u):
        m, x = u // 2, par(u)
        return remote(g2s.at[m, :, x], g2d.at[k, m], gd_send.at[u], gd_recv.at[k, m], down2 + x)

    def g2d_arrival(u):
        m, p = u // 2, par(u)
        return remote(g2s.at[m, :, p], g2d.at[p, m], gd_send.at[u], gd_recv.at[p, m], down2)

    def g1_copy(u):
        m = u // 2
        x = par(u)
        return remote(g1s.at[m, x], g1r.at[k, m], g1_send.at[u], g1_recv.at[k, m], down + x)

    def g1_arrival(u):
        m = u // 2
        p = par(u)
        return remote(g1s.at[m, p], g1r.at[p, m], g1_send.at[u], g1_recv.at[p, m], down)

    x_kv = remote(kv_x, kraw.at[4 + k], x_send.at[0], x_recv.at[0], partner)
    x_q = remote(qx, qf.at[k], x_send.at[1], x_recv.at[1], partner)
    x_g = remote(gx, gf.at[k], x_send.at[2], x_recv.at[2], partner)
    x_st = remote(stx, st.at[k], x_send.at[3], x_recv.at[3], partner)
    g0_copy = remote(acc_l.at[oth], g0r, x_send.at[4], x_recv.at[4], partner)

    def kv_wait(m, i):
        for e in range(2):
            kv_loads[(m * 2 + i) * 2 + e].wait()

    def flat(val):
        return val.reshape(val.shape[0] * 2, HD)

    def split(m):
        for i, dst in enumerate((kraw.at[4 + k, m], kv_x.at[m])):
            kv_wait(m, i)
            for e in range(2):
                kf[e] = flat(kin[i, m, e]).astype(F32)
                for j in range(2):
                    dst[e, j] = kf[e, pl.ds(j, TC, stride=2), :].astype(BF)

    for m in range(NC):
        split(m)
        if m < 2:
            own_copy(2 * m).start()
            own_copy(2 * m + 1).start()
    x_kv.start()
    for raw, near, far, first, copy in ((qraw, qf, qx, 0, x_q), (graw, gf, gx, 4, x_g)):
        for j in range(2):
            in_loads[first + 2 + j].wait()
            far[j] = flat(raw[1, j])
        copy.start()
        for j in range(2):
            in_loads[first + j].wait()
            near[k, j] = flat(raw[0, j])
    for i in range(8, 13):
        in_loads[i].wait()

    lse = lse_s[...] * LOG2E
    hi = lse.astype(BF)
    rest = lse - hi.astype(F32)
    mid = rest.astype(BF)
    low = (rest - mid.astype(F32)).astype(BF)
    parts = jnp.concatenate([hi.astype(F32), mid.astype(F32), low.astype(F32), jnp.zeros_like(lse)], 0).astype(BF)
    row = lax.broadcasted_iota(jnp.int32, (T, 2 * T), 0)
    col = lax.broadcasted_iota(jnp.int32, (T, 2 * T), 1)
    wide = []
    for e in range(2):
        place = jnp.where(col == 2 * row + e, 1.0, 0.0).astype(BF)
        r = dot_nn(parts, place)
        wide.append(r[0:8] + r[8:16] + r[16:24])
    lse_w = [wide[0][2 * i : 2 * i + 1] + wide[1][2 * i + 1 : 2 * i + 2] for i in range(4)]
    ones = jnp.ones((8, HD), BF)

    def delta_of(a, b):
        prod = a.astype(F32) * b.astype(F32)
        top = prod.astype(BF)
        left = (prod - top.astype(F32)).astype(BF)
        return (dot_nt(ones, top) + dot_nt(ones, left))[0:1]

    no_1 = jnp.where(chip < 1, FAR, 0.0).astype(F32)
    no_2 = jnp.where(chip < 2, FAR, 0.0).astype(F32)
    for j in range(2):
        for which in range(2):
            if which == 0:
                dst, dl = st.at[k, j], delta_of(gf[k, j], flat(ob[0, j]))
            else:
                dst, dl = stx.at[j], delta_of(gx[j], flat(ob[1, j]))
            if which == 0:
                lw = jnp.where(k == 0, lse_w[j], lse_w[2 + j])
            else:
                lw = jnp.where(k == 0, lse_w[2 + j], lse_w[j])
            dst[0:1, :] = lw
            dst[1:2, :] = dl
            dst[2:3, :] = lw + no_1
            dst[3:4, :] = lw + no_2
            dst[4:8, :] = jnp.zeros((4, 2 * T), F32)
    x_st.start()
    dq_t[...] = jnp.zeros_like(dq_t)

    def flip(b):
        for j in range(2):
            qt[b, j] = qf[b, j].T
            gt[b, j] = gf[b, j].T

    def tile(kc, vc, b, j, lo, norm_row, mask):
        q, g = qf[b, j, lo:, :], gf[b, j, lo:, :]
        sc = dot_nn(kc, qt[b, j, :, lo:])
        dp = dot_nn(vc, gt[b, j, :, lo:])
        p = jnp.exp2(sc * (SCALE * LOG2E) - st[b, j, norm_row : norm_row + 1, lo:])
        if mask is not None:
            p = jnp.where(mask, p, 0.0)
        dv = dot_nn(p.astype(BF), g)
        ds = (p * (dp - st[b, j, 1:2, lo:])).astype(BF)
        dk = dot_nn(ds, q)
        dq_t[b, j, :, lo:] += dot_tn(kc, ds)
        return dk, dv

    def keys(j, *parts):
        return [jnp.concatenate([kraw[x, m, e, j] for x, m in parts], 0) for e in range(2)]

    def heads(body):
        lax.fori_loop(0, 2, lambda j, c: (body(j), c)[1], 0)

    def grid2(rows, lo):
        row = lax.broadcasted_iota(jnp.int32, (rows, 2 * T - lo), 0)
        tok = (lo + lax.broadcasted_iota(jnp.int32, (rows, 2 * T - lo), 1)) // 2
        return row, tok

    R = 2 * TC

    def local_causal(x):
        for h in range(NC // 2):
            lo = 2 * h * R

            def body(j):
                row, tok = grid2(R, lo)
                kc, vc = keys(j, (4 + x, 2 * h), (4 + x, 2 * h + 1))
                dk, dv = tile(kc, vc, x, j, lo, 0, tok >= row + h * R)
                acc_l[x, 0, j, pl.ds(h * R, R), :] = dk
                acc_l[x, 1, j, pl.ds(h * R, R), :] = dv

            heads(body)

    def local_full():
        for h in range(NC // 2):

            def body(j):
                kc, vc = keys(j, (4, 2 * h), (4, 2 * h + 1))
                dk, dv = tile(kc, vc, 1, j, 0, 0, None)
                acc_l[0, 0, j, pl.ds(h * R, R), :] += dk
                acc_l[0, 1, j, pl.ds(h * R, R), :] += dv

            heads(body)

    def near(m):
        def body(j):
            kc, vc = keys(j, (2, m), (3, m))
            dk0, dv0 = tile(kc, vc, 0, j, 0, 2, None)
            dk1, dv1 = tile(kc, vc, 1, j, 0, 2, None)
            acc_h[m, 0, j] = dk0 + dk1
            acc_h[m, 1, j] = dv0 + dv1

        heads(body)

    def far(m):
        def body(j):
            row, tok = grid2(R, 0)
            kc, vc = keys(j, (0, m), (1, m))
            dk0, dv0 = tile(kc, vc, 0, j, 0, 3, (row >= TC) | (row + m * TC > tok))
            row, tok = grid2(TC, 0)
            dk1, dv1 = tile(kc[TC:], vc[TC:], 1, j, 0, 3, row + m * TC > tok)
            g2s[m, j, 0, 0] = dk0[:TC].astype(BF)
            g2s[m, j, 0, 1] = dv0[:TC].astype(BF)
            g2s[m, j, 1, 0] = (dk0[TC:] + dk1).astype(BF)
            g2s[m, j, 1, 1] = (dv0[TC:] + dv1).astype(BF)
            if m not in DIRECT_G:
                g2_copy(m, j).start()

        heads(body)

    def near_finish(m):
        for j in range(2):
            if m not in DIRECT_G:
                g2_copy(m, j).wait_recv()
            for x in range(2):
                for e in range(2):
                    val = acc_h[m, e, j, x * TC : (x + 1) * TC]
                    if m not in DIRECT_G:
                        val = val + g2r[m, j, x, e].astype(F32)
                    g1s[m, x, e, j] = val.astype(BF)

    outs = []

    def final_unit(u):
        m, p = u // 2, par(u)
        rows = pl.ds(m * TC, TC)
        for e in range(2):
            for j in range(2):
                mine = acc_l[k, e, j, rows, :] if u % 2 == 0 else g0r[e, j, rows, :]
                val = mine + g1r[p, m, e, j].astype(F32)
                if m in DIRECT_G:
                    val = val + g2d[p, m, j, e].astype(F32)
                if e == 0:
                    val = val * SCALE
                fi[e, pl.ds(j, TC, stride=2), :] = val
            fo[u, e] = fi[e].astype(BF)
            dst = (gk_out, gv_out)[e]
            c = pltpu.make_async_copy(fo.at[u, e], dst.at[p, pl.ds(2 * m * TC, 2 * TC)], out_sem.at[2 * u + e])
            c.start()
            outs.append(c)

    def arrive(u):
        own_arrival(u).wait_recv()
        if u // 2 not in DIRECT_KV:
            relay_copy(u).start()

    def own_send(m):
        own_copy(2 * m).start()
        own_copy(2 * m + 1).start()

    def far_step(m):
        relay_copy(2 * m).wait_recv()
        relay_copy(2 * m + 1).wait_recv()
        far(m)
        if m in DIRECT_G:
            g2d_copy(2 * m).start()
            g2d_copy(2 * m + 1).start()

    def near_step(m):
        near_finish(m)
        g1_copy(2 * m).start()
        g1_copy(2 * m + 1).start()

    def final_step(u):
        g1_arrival(u).wait_recv()
        if u // 2 in DIRECT_G:
            g2d_arrival(u).wait_recv()
        final_unit(u)

    def from_partner():
        for c in (x_kv, x_q, x_g, x_st):
            c.wait_recv()

    def local_rest():
        local_full()
        g0_copy.start()

    dq_copies = []

    def query_grads():
        for j in range(2):
            for b in (oth, k):
                dqs[b, j] = (dq_t[b, j].T * SCALE).astype(BF)
            c = remote(dqs.at[oth, j], gq_out.at[2 * k + j], dq_send.at[j], dq_recv.at[j], partner)
            c.start()
            dq_copies.append(c)
            c = pltpu.make_async_copy(dqs.at[k, j], gq_out.at[2 * k + j], out_sem.at[2 * NU + j])
            c.start()
            outs.append(c)

    steps = {
        "flip0": lambda: flip(k), "flip1": lambda: flip(oth),
        "L0": lambda: local_causal(k), "L1": lambda: local_causal(oth), "LF": local_rest,
        "X": from_partner, "Q": lambda: g0_copy.wait_recv(), "D": query_grads,
    }
    by_index = {"A": arrive, "o": own_send, "N": near, "F": far_step, "S": near_step, "Z": final_step}
    for word in PLAN:
        if word in steps:
            steps[word]()
        else:
            by_index[word[0]](int(word[1:]))

    for u in range(NU):
        own_copy(u).wait_send()
        (direct_copy if u // 2 in DIRECT_KV else relay_copy)(u).wait_send()
        g1_copy(u).wait_send()
        if u // 2 in DIRECT_G:
            g2d_copy(u).wait_send()
    for m in range(NC):
        if m not in DIRECT_G:
            for j in range(2):
                g2_copy(m, j).wait_send()
    for c in (x_kv, x_q, x_g, x_st, g0_copy):
        c.wait_send()
    for c in dq_copies:
        c.wait()
    for c in outs:
        c.wait()


def deliver(q_in, k_in, v_in, q_out, k_out, v_out, sem):
    copies = []
    for src, dst in ((q_in, q_out), (k_in, k_out), (v_in, v_out)):
        for p in range(src.shape[0]):
            copies.append(pltpu.make_async_copy(src.at[p], dst.at[:, p], sem.at[len(copies)]))
    for c in copies:
        c.start()
    for c in copies:
        c.wait()


def shards(n, queries, key_rows, value_rows, attn_output, grad_output, log_norm):
    heads4 = (T, 4, 2, HD)
    heads2 = (T, 2, 2, HD)
    anym = pl.BlockSpec(memory_space=pl.ANY)
    dma = pltpu.SemaphoreType.DMA
    vm = pltpu.VMEM
    pair = (T, 2, HD)
    scratch = [
        vm((2, NC, 2, TC, 2, HD), BF),
        vm((6, NC, 2, 2, TC, HD), BF),
        vm((NC, 2, 2, TC, HD), BF),
        vm((2, 2) + pair, BF),
        vm((2, 2) + pair, BF),
        vm((2, 2) + pair, BF),
        vm((2, 2, 2 * T, HD), BF),
        vm((2, 2, 2 * T, HD), BF),
        vm((2, 2, HD, 2 * T), BF),
        vm((2, 2, HD, 2 * T), BF),
        vm((2, 2 * T, HD), BF),
        vm((2, 2 * T, HD), BF),
        vm((8, T), F32),
        vm((2, 2, 8, 2 * T), F32),
        vm((2, 8, 2 * T), F32),
        vm((2, 2 * TC, HD), F32),
        vm((NC, 2, 2, 2 * TC, HD), F32),
        vm((2, 2, 2, T, HD), F32),
        vm((2, 2, HD, 2 * T), F32),
        vm((2, 2, 2 * T, HD), BF),
        vm((NC, 2, 2, 2, TC, HD), BF),
        vm((NC, 2, 2, 2, TC, HD), BF),
        vm((NC, 2, 2, 2, TC, HD), BF),
        vm((2, NC, 2, 2, TC, HD), BF),
        vm((2, NC, 2, 2, TC, HD), BF),
        vm((2, 2, T, HD), F32),
        vm((2, 2 * TC, HD), F32),
        vm((NU, 2, 2 * TC, HD), BF),
        dma((NC, 2, 2)),
        dma((13,)),
        dma((NU,)), dma((2, NC)),
        dma((NU,)), dma((2, NC)),
        dma((NC, 2)), dma((NC, 2)),
        dma((NU,)), dma((2, NC)),
        dma((NU,)), dma((2, NC)),
        dma((5,)), dma((5,)),
        dma((2,)), dma((2,)),
        dma((2 * NU + 2,)),
    ]
    gq, gk, gv = pl.pallas_call(
        functools.partial(kernel, n),
        out_shape=(
            jax.ShapeDtypeStruct((4, 2 * T, HD), BF),
            jax.ShapeDtypeStruct((2, 2 * T, HD), BF),
            jax.ShapeDtypeStruct((2, 2 * T, HD), BF),
        ),
        in_specs=[pl.BlockSpec(memory_space=pltpu.HBM)] * 6,
        out_specs=(anym,) * 3,
        scratch_shapes=scratch,
        compiler_params=pltpu.CompilerParams(
            collective_id=0, has_side_effects=True, vmem_limit_bytes=VMEM_KIB << 10
        ),
    )(
        *(
            pltpu.with_memory_space_constraint(a, pltpu.HBM)
            for a in (
                queries.reshape(heads4),
                key_rows.reshape(heads2),
                value_rows.reshape(heads2),
                attn_output.reshape(heads4),
                grad_output.reshape(heads4),
                log_norm,
            )
        )
    )
    gq, gk, gv = pl.pallas_call(
        deliver,
        out_shape=tuple(jax.ShapeDtypeStruct(shape, BF) for shape in (heads4, heads2, heads2)),
        in_specs=[anym] * 3,
        out_specs=(pl.BlockSpec(memory_space=pltpu.HBM),) * 3,
        scratch_shapes=[dma((8,))],
        compiler_params=pltpu.CompilerParams(vmem_limit_bytes=1 << 20),
    )(*(a.reshape((a.shape[0],) + pair) for a in (gq, gk, gv)))
    return (
        gq.reshape(queries.shape),
        gk.reshape(key_rows.shape),
        gv.reshape(value_rows.shape),
    )


def solution(mesh):
    wide = P("seq", None, None)
    return jax.shard_map(
        functools.partial(shards, mesh.shape["seq"]),
        mesh=mesh,
        in_specs=(wide, wide, wide, wide, wide, P(None, "seq")),
        out_specs=(wide, wide, wide),
        check_vma=False,
    )
```

```python
import functools
import math

import jax
import jax.numpy as jnp
from jax import lax
from jax.experimental import pallas as pl
from jax.experimental.pallas import tpu as pltpu
from jax.sharding import PartitionSpec as P

MESH = pl.DeviceIdType.MESH
BF = jnp.bfloat16
F32 = jnp.float32
SCALE = 168.0 ** (-0.5)
LOG2E = math.log2(math.e)
T = 256
HD = 128
NC = 4
TC = T // NC
NU = 2 * NC
FAR = 1e30
VMEM_KIB = 24 << 10
VIA = 3
DIRECT_G = ()
PLAN = ('A0', 'A1', 'V', 'flip0', 'L0', 'X', 'flip1', 'N0', 'A2', 'F0', 'A3', 'N1', 'A4', 'F3', 'F1', 'S0', 'A5', 'L1', 'N2', 'A6', 'S1', 'F2', 'A7', 'N3', 'S3', 'LF', 'D', 'S2', 'Q', 'Z0', 'Z1', 'Z2', 'Z3', 'Z6', 'Z7', 'Z4', 'Z5')


def dot_nt(a, b):
    return lax.dot_general(a, b, (((1,), (1,)), ((), ())), preferred_element_type=F32)


def dot_nn(a, b):
    return lax.dot_general(a, b, (((1,), (0,)), ((), ())), preferred_element_type=F32)


def dot_tn(a, b):
    return lax.dot_general(a, b, (((0,), (0,)), ((), ())), preferred_element_type=F32)


def kernel(
    n,
    q_hbm, k_hbm, v_hbm, o_hbm, g_hbm, lse_hbm,
    gq_out, gk_out, gv_out,
    kin, kraw, kv_x, via_b, qraw, graw, ob, qf, gf, qt, gt, qx, gx, lse_s, st, stx, kf,
    acc_h, acc_l, dq_t, dqs, g2s, g2r, g1s, g1r, g2d, g0r, fi, fo,
    kv_ld, in_ld,
    o_send, o_recv, via_send, via_recv, r_send, r_recv, g2_send, g2_recv, g1_send, g1_recv, gd_send, gd_recv,
    x_send, x_recv, dq_send, dq_recv, out_sem,
):
    me = lax.axis_index("seq")
    k = lax.rem(me, 2)
    oth = 1 - k
    chip = lax.div(me, 2)
    up = lax.rem(me - k + 2, n)
    down = lax.rem(me - k + n - 2, n)
    up2 = lax.rem(me - k + 4, n)
    down2 = lax.rem(me - k + n - 4, n)
    up3 = lax.rem(me - k + 6, n)
    down3 = lax.rem(me - k + n - 6, n)
    y = lax.rem(chip, 4)
    via_dev = jnp.where(y == 0, up3, down)
    onward = jnp.where(y == 3, down, up3)
    partner = me - k + oth

    def remote(src, dst, ssem, rsem, dev):
        return pltpu.make_async_remote_copy(
            src_ref=src, dst_ref=dst, send_sem=ssem, recv_sem=rsem,
            device_id=(dev,), device_id_type=MESH,
        )

    def par(u):
        return k if u % 2 == 0 else oth

    kv_loads = []
    for m in range(NC):
        rows = pl.ds(m * TC, TC)
        for i, pair in enumerate((k, oth)):
            for e, src in enumerate((k_hbm, v_hbm)):
                kv_loads.append(
                    pltpu.make_async_copy(src.at[rows, pair], kin.at[i, m, e], kv_ld.at[m, i, e])
                )
    for c in kv_loads:
        c.start()
    in_loads = []
    s = 0
    for src, dst2 in ((q_hbm, qraw), (g_hbm, graw), (o_hbm, ob)):
        for i, base in enumerate((k, oth)):
            for j in range(2):
                in_loads.append(
                    pltpu.make_async_copy(src.at[:, 2 * base + j], dst2.at[i, j], in_ld.at[s])
                )
                s += 1
    in_loads.append(pltpu.make_async_copy(lse_hbm, lse_s, in_ld.at[s]))
    for c in in_loads:
        c.start()

    bar = pltpu.get_barrier_semaphore()
    for dev in (up, up + 1, down, down + 1, up2, up2 + 1, down2, down2 + 1, up3, up3 + 1, down3, down3 + 1, partner):
        pl.semaphore_signal(bar, inc=1, device_id=(dev,), device_id_type=MESH)
    pl.semaphore_wait(bar, 13)

    def own_copy(u):
        m = u // 2
        src = kraw.at[4 + k, m] if u % 2 == 0 else kv_x.at[m]
        dev = up + par(u)
        return remote(src, kraw.at[2 + k, m], o_send.at[u], o_recv.at[k, m], dev)

    def own_arrival(u):
        m = u // 2
        x = par(u)
        return remote(kraw.at[2 + x, m], kraw.at[2 + x, m], o_send.at[u], o_recv.at[x, m], up)

    def via_copy(u):
        src = kraw.at[4 + k, VIA] if u % 2 == 0 else kv_x.at[VIA]
        return remote(src, via_b.at[k], via_send.at[u % 2], via_recv.at[k], via_dev + par(u))

    def via_onward(u):
        x = par(u)
        return remote(via_b.at[x], kraw.at[x, VIA], r_send.at[u], r_recv.at[x, VIA], onward + k)

    def via_arrival(u):
        x = par(u)
        return remote(via_b.at[x], via_b.at[x], via_send.at[u % 2], via_recv.at[x], via_dev)

    def relay_copy(u):
        m = u // 2
        x = par(u)
        return remote(kraw.at[2 + x, m], kraw.at[x, m], r_send.at[u], r_recv.at[x, m], up + k)

    def g2_copy(m, j):
        return remote(g2s.at[m, j], g2r.at[m, j], g2_send.at[m, j], g2_recv.at[m, j], down + k)

    def g2d_copy(u):
        m, x = u // 2, par(u)
        return remote(g2s.at[m, :, x], g2d.at[k, m], gd_send.at[u], gd_recv.at[k, m], down2 + x)

    def g2d_arrival(u):
        m, p = u // 2, par(u)
        return remote(g2s.at[m, :, p], g2d.at[p, m], gd_send.at[u], gd_recv.at[p, m], down2)

    def g1_copy(u):
        m = u // 2
        x = par(u)
        return remote(g1s.at[m, x], g1r.at[k, m], g1_send.at[u], g1_recv.at[k, m], down + x)

    def g1_arrival(u):
        m = u // 2
        p = par(u)
        return remote(g1s.at[m, p], g1r.at[p, m], g1_send.at[u], g1_recv.at[p, m], down)

    x_kv = remote(kv_x, kraw.at[4 + k], x_send.at[0], x_recv.at[0], partner)
    x_q = remote(qx, qf.at[k], x_send.at[1], x_recv.at[1], partner)
    x_g = remote(gx, gf.at[k], x_send.at[2], x_recv.at[2], partner)
    x_st = remote(stx, st.at[k], x_send.at[3], x_recv.at[3], partner)
    g0_copy = remote(acc_l.at[oth], g0r, x_send.at[4], x_recv.at[4], partner)

    def kv_wait(m, i):
        for e in range(2):
            kv_loads[(m * 2 + i) * 2 + e].wait()

    def flat(val):
        return val.reshape(val.shape[0] * 2, HD)

    def split(m):
        for i, dst in enumerate((kraw.at[4 + k, m], kv_x.at[m])):
            kv_wait(m, i)
            for e in range(2):
                kf[e] = flat(kin[i, m, e]).astype(F32)
                for j in range(2):
                    dst[e, j] = kf[e, pl.ds(j, TC, stride=2), :].astype(BF)

    for m in (0, VIA, 1, 2):
        split(m)
        for u in (2 * m, 2 * m + 1):
            if m == 0:
                own_copy(u).start()
            elif m == VIA:
                via_copy(u).start()
    x_kv.start()
    for raw, near, far, first, copy in ((qraw, qf, qx, 0, x_q), (graw, gf, gx, 4, x_g)):
        for j in range(2):
            in_loads[first + 2 + j].wait()
            far[j] = flat(raw[1, j])
        copy.start()
        for j in range(2):
            in_loads[first + j].wait()
            near[k, j] = flat(raw[0, j])
    for i in range(8, 13):
        in_loads[i].wait()

    lse = lse_s[...] * LOG2E
    hi = lse.astype(BF)
    rest = lse - hi.astype(F32)
    mid = rest.astype(BF)
    low = (rest - mid.astype(F32)).astype(BF)
    parts = jnp.concatenate([hi.astype(F32), mid.astype(F32), low.astype(F32), jnp.zeros_like(lse)], 0).astype(BF)
    row = lax.broadcasted_iota(jnp.int32, (T, 2 * T), 0)
    col = lax.broadcasted_iota(jnp.int32, (T, 2 * T), 1)
    wide = []
    for e in range(2):
        place = jnp.where(col == 2 * row + e, 1.0, 0.0).astype(BF)
        r = dot_nn(parts, place)
        wide.append(r[0:8] + r[8:16] + r[16:24])
    lse_w = [wide[0][2 * i : 2 * i + 1] + wide[1][2 * i + 1 : 2 * i + 2] for i in range(4)]
    ones = jnp.ones((8, HD), BF)

    def delta_of(a, b):
        prod = a.astype(F32) * b.astype(F32)
        top = prod.astype(BF)
        left = (prod - top.astype(F32)).astype(BF)
        return (dot_nt(ones, top) + dot_nt(ones, left))[0:1]

    no_1 = jnp.where(chip < 1, FAR, 0.0).astype(F32)
    no_2 = jnp.where(chip < 2, FAR, 0.0).astype(F32)
    for j in range(2):
        for which in range(2):
            if which == 0:
                dst, dl = st.at[k, j], delta_of(gf[k, j], flat(ob[0, j]))
            else:
                dst, dl = stx.at[j], delta_of(gx[j], flat(ob[1, j]))
            if which == 0:
                lw = jnp.where(k == 0, lse_w[j], lse_w[2 + j])
            else:
                lw = jnp.where(k == 0, lse_w[2 + j], lse_w[j])
            dst[0:1, :] = lw
            dst[1:2, :] = dl
            dst[2:3, :] = lw + no_1
            dst[3:4, :] = lw + no_2
            dst[4:8, :] = jnp.zeros((4, 2 * T), F32)
    x_st.start()
    dq_t[...] = jnp.zeros_like(dq_t)

    def flip(b):
        for j in range(2):
            qt[b, j] = qf[b, j].T
            gt[b, j] = gf[b, j].T

    def tile(kc, vc, b, j, lo, norm_row, mask):
        q, g = qf[b, j, lo:, :], gf[b, j, lo:, :]
        sc = dot_nn(kc, qt[b, j, :, lo:])
        dp = dot_nn(vc, gt[b, j, :, lo:])
        p = jnp.exp2(sc * (SCALE * LOG2E) - st[b, j, norm_row : norm_row + 1, lo:])
        if mask is not None:
            p = jnp.where(mask, p, 0.0)
        dv = dot_nn(p.astype(BF), g)
        ds = (p * (dp - st[b, j, 1:2, lo:])).astype(BF)
        dk = dot_nn(ds, q)
        dq_t[b, j, :, lo:] += dot_tn(kc, ds)
        return dk, dv

    def keys(j, *parts):
        return [jnp.concatenate([kraw[x, m, e, j] for x, m in parts], 0) for e in range(2)]

    def heads(body):
        lax.fori_loop(0, 2, lambda j, c: (body(j), c)[1], 0)

    def grid2(rows, lo):
        row = lax.broadcasted_iota(jnp.int32, (rows, 2 * T - lo), 0)
        tok = (lo + lax.broadcasted_iota(jnp.int32, (rows, 2 * T - lo), 1)) // 2
        return row, tok

    R = 2 * TC

    def local_causal(x):
        for h in range(NC // 2):
            lo = 2 * h * R

            def body(j):
                row, tok = grid2(R, lo)
                kc, vc = keys(j, (4 + x, 2 * h), (4 + x, 2 * h + 1))
                dk, dv = tile(kc, vc, x, j, lo, 0, tok >= row + h * R)
                acc_l[x, 0, j, pl.ds(h * R, R), :] = dk
                acc_l[x, 1, j, pl.ds(h * R, R), :] = dv

            heads(body)

    def local_full():
        for h in range(NC // 2):

            def body(j):
                kc, vc = keys(j, (4, 2 * h), (4, 2 * h + 1))
                dk, dv = tile(kc, vc, 1, j, 0, 0, None)
                acc_l[0, 0, j, pl.ds(h * R, R), :] += dk
                acc_l[0, 1, j, pl.ds(h * R, R), :] += dv

            heads(body)

    def near(m):
        def body(j):
            kc, vc = keys(j, (2, m), (3, m))
            dk0, dv0 = tile(kc, vc, 0, j, 0, 2, None)
            dk1, dv1 = tile(kc, vc, 1, j, 0, 2, None)
            acc_h[m, 0, j] = dk0 + dk1
            acc_h[m, 1, j] = dv0 + dv1

        heads(body)

    def far(m):
        def body(j):
            row, tok = grid2(R, 0)
            kc, vc = keys(j, (0, m), (1, m))
            dk0, dv0 = tile(kc, vc, 0, j, 0, 3, (row >= TC) | (row + m * TC > tok))
            row, tok = grid2(TC, 0)
            dk1, dv1 = tile(kc[TC:], vc[TC:], 1, j, 0, 3, row + m * TC > tok)
            g2s[m, j, 0, 0] = dk0[:TC].astype(BF)
            g2s[m, j, 0, 1] = dv0[:TC].astype(BF)
            g2s[m, j, 1, 0] = (dk0[TC:] + dk1).astype(BF)
            g2s[m, j, 1, 1] = (dv0[TC:] + dv1).astype(BF)
            if m not in DIRECT_G:
                g2_copy(m, j).start()

        heads(body)

    def near_finish(m):
        for j in range(2):
            if m not in DIRECT_G:
                g2_copy(m, j).wait_recv()
            for x in range(2):
                for e in range(2):
                    val = acc_h[m, e, j, x * TC : (x + 1) * TC]
                    if m not in DIRECT_G:
                        val = val + g2r[m, j, x, e].astype(F32)
                    g1s[m, x, e, j] = val.astype(BF)

    outs = []

    def final_unit(u):
        m, p = u // 2, par(u)
        rows = pl.ds(m * TC, TC)
        for e in range(2):
            for j in range(2):
                mine = acc_l[k, e, j, rows, :] if u % 2 == 0 else g0r[e, j, rows, :]
                val = mine + g1r[p, m, e, j].astype(F32)
                if m in DIRECT_G:
                    val = val + g2d[p, m, j, e].astype(F32)
                if e == 0:
                    val = val * SCALE
                fi[e, pl.ds(j, TC, stride=2), :] = val
            fo[u, e] = fi[e].astype(BF)
            dst = (gk_out, gv_out)[e]
            c = pltpu.make_async_copy(fo.at[u, e], dst.at[p, pl.ds(2 * m * TC, 2 * TC)], out_sem.at[2 * u + e])
            c.start()
            outs.append(c)

    def arrive(u):
        own_arrival(u).wait_recv()
        if u // 2 != VIA:
            relay_copy(u).start()
        if u + 2 < NU:
            own_copy(u + 2).start()

    def pass_on():
        for u in (2 * VIA, 2 * VIA + 1):
            via_arrival(u).wait_recv()
            via_onward(u).start()

    def far_step(m):
        relay_copy(2 * m).wait_recv()
        relay_copy(2 * m + 1).wait_recv()
        far(m)
        if m in DIRECT_G:
            g2d_copy(2 * m).start()
            g2d_copy(2 * m + 1).start()

    def near_step(m):
        near_finish(m)
        g1_copy(2 * m).start()
        g1_copy(2 * m + 1).start()

    def final_step(u):
        g1_arrival(u).wait_recv()
        if u // 2 in DIRECT_G:
            g2d_arrival(u).wait_recv()
        final_unit(u)

    def from_partner():
        for c in (x_kv, x_q, x_g, x_st):
            c.wait_recv()

    def local_rest():
        local_full()
        g0_copy.start()

    dq_copies = []

    def query_grads():
        for j in range(2):
            for b in (oth, k):
                dqs[b, j] = (dq_t[b, j].T * SCALE).astype(BF)
            c = remote(dqs.at[oth, j], gq_out.at[2 * k + j], dq_send.at[j], dq_recv.at[j], partner)
            c.start()
            dq_copies.append(c)
            c = pltpu.make_async_copy(dqs.at[k, j], gq_out.at[2 * k + j], out_sem.at[2 * NU + j])
            c.start()
            outs.append(c)

    steps = {
        "flip0": lambda: flip(k), "flip1": lambda: flip(oth),
        "L0": lambda: local_causal(k), "L1": lambda: local_causal(oth), "LF": local_rest,
        "X": from_partner, "V": pass_on, "Q": lambda: g0_copy.wait_recv(), "D": query_grads,
    }
    by_index = {"A": arrive, "N": near, "F": far_step, "S": near_step, "Z": final_step}
    for word in PLAN:
        if word in steps:
            steps[word]()
        else:
            by_index[word[0]](int(word[1:]))

    for u in range(NU):
        own_copy(u).wait_send()
        (via_onward if u // 2 == VIA else relay_copy)(u).wait_send()
        if u // 2 == VIA:
            via_copy(u).wait_send()
        g1_copy(u).wait_send()
        if u // 2 in DIRECT_G:
            g2d_copy(u).wait_send()
    for m in range(NC):
        if m not in DIRECT_G:
            for j in range(2):
                g2_copy(m, j).wait_send()
    for c in (x_kv, x_q, x_g, x_st, g0_copy):
        c.wait_send()
    for c in dq_copies:
        c.wait()
    for c in outs:
        c.wait()


def deliver(q_in, k_in, v_in, q_out, k_out, v_out, sem):
    copies = []
    for src, dst in ((q_in, q_out), (k_in, k_out), (v_in, v_out)):
        for p in range(src.shape[0]):
            copies.append(pltpu.make_async_copy(src.at[p], dst.at[:, p], sem.at[len(copies)]))
    for c in copies:
        c.start()
    for c in copies:
        c.wait()


def shards(n, queries, key_rows, value_rows, attn_output, grad_output, log_norm):
    heads4 = (T, 4, 2, HD)
    heads2 = (T, 2, 2, HD)
    anym = pl.BlockSpec(memory_space=pl.ANY)
    dma = pltpu.SemaphoreType.DMA
    vm = pltpu.VMEM
    pair = (T, 2, HD)
    scratch = [
        vm((2, NC, 2, TC, 2, HD), BF),
        vm((6, NC, 2, 2, TC, HD), BF),
        vm((NC, 2, 2, TC, HD), BF),
        vm((2, 2, 2, TC, HD), BF),
        vm((2, 2) + pair, BF),
        vm((2, 2) + pair, BF),
        vm((2, 2) + pair, BF),
        vm((2, 2, 2 * T, HD), BF),
        vm((2, 2, 2 * T, HD), BF),
        vm((2, 2, HD, 2 * T), BF),
        vm((2, 2, HD, 2 * T), BF),
        vm((2, 2 * T, HD), BF),
        vm((2, 2 * T, HD), BF),
        vm((8, T), F32),
        vm((2, 2, 8, 2 * T), F32),
        vm((2, 8, 2 * T), F32),
        vm((2, 2 * TC, HD), F32),
        vm((NC, 2, 2, 2 * TC, HD), F32),
        vm((2, 2, 2, T, HD), F32),
        vm((2, 2, HD, 2 * T), F32),
        vm((2, 2, 2 * T, HD), BF),
        vm((NC, 2, 2, 2, TC, HD), BF),
        vm((NC, 2, 2, 2, TC, HD), BF),
        vm((NC, 2, 2, 2, TC, HD), BF),
        vm((2, NC, 2, 2, TC, HD), BF),
        vm((2, NC, 2, 2, TC, HD), BF),
        vm((2, 2, T, HD), F32),
        vm((2, 2 * TC, HD), F32),
        vm((NU, 2, 2 * TC, HD), BF),
        dma((NC, 2, 2)),
        dma((13,)),
        dma((NU,)), dma((2, NC)),
        dma((2,)), dma((2,)),
        dma((NU,)), dma((2, NC)),
        dma((NC, 2)), dma((NC, 2)),
        dma((NU,)), dma((2, NC)),
        dma((NU,)), dma((2, NC)),
        dma((5,)), dma((5,)),
        dma((2,)), dma((2,)),
        dma((2 * NU + 2,)),
    ]
    gq, gk, gv = pl.pallas_call(
        functools.partial(kernel, n),
        out_shape=(
            jax.ShapeDtypeStruct((4, 2 * T, HD), BF),
            jax.ShapeDtypeStruct((2, 2 * T, HD), BF),
            jax.ShapeDtypeStruct((2, 2 * T, HD), BF),
        ),
        in_specs=[pl.BlockSpec(memory_space=pltpu.HBM)] * 6,
        out_specs=(anym,) * 3,
        scratch_shapes=scratch,
        compiler_params=pltpu.CompilerParams(
            collective_id=0, has_side_effects=True, vmem_limit_bytes=VMEM_KIB << 10
        ),
    )(
        *(
            pltpu.with_memory_space_constraint(a, pltpu.HBM)
            for a in (
                queries.reshape(heads4),
                key_rows.reshape(heads2),
                value_rows.reshape(heads2),
                attn_output.reshape(heads4),
                grad_output.reshape(heads4),
                log_norm,
            )
        )
    )
    gq, gk, gv = pl.pallas_call(
        deliver,
        out_shape=tuple(jax.ShapeDtypeStruct(shape, BF) for shape in (heads4, heads2, heads2)),
        in_specs=[anym] * 3,
        out_specs=(pl.BlockSpec(memory_space=pltpu.HBM),) * 3,
        scratch_shapes=[dma((8,))],
        compiler_params=pltpu.CompilerParams(vmem_limit_bytes=1 << 20),
    )(*(a.reshape((a.shape[0],) + pair) for a in (gq, gk, gv)))
    return (
        gq.reshape(queries.shape),
        gk.reshape(key_rows.shape),
        gv.reshape(value_rows.shape),
    )


def solution(mesh):
    wide = P("seq", None, None)
    return jax.shard_map(
        functools.partial(shards, mesh.shape["seq"]),
        mesh=mesh,
        in_specs=(wide, wide, wide, wide, wide, P(None, "seq")),
        out_specs=(wide, wide, wide),
        check_vma=False,
    )
```

```python
import functools
import math

import jax
import jax.numpy as jnp
from jax import lax
from jax.experimental import pallas as pl
from jax.experimental.pallas import tpu as pltpu
from jax.sharding import PartitionSpec as P

MESH = pl.DeviceIdType.MESH
BF = jnp.bfloat16
F32 = jnp.float32
SCALE = 168.0 ** (-0.5)
LOG2E = math.log2(math.e)
T = 256
HD = 128
NC = 4
TC = T // NC
NU = 2 * NC
FAR = 1e30
VMEM_KIB = 24 << 10
VIA = 3
PLAN = (
    "G", "T", "A0", "A1", "V", "flip0", "L0", "X", "flip1", "N0", "A2", "F0", "A3", "N1",
    "A4", "F3", "F1", "S0", "A5", "L1", "N2", "A6", "S1", "F2", "A7", "N3", "S3", "LF",
    "D", "S2", "Q", "Z0", "Z1", "Z2", "Z3", "Z6", "Z7", "Z4", "Z5",
)


def dot_nt(a, b):
    return lax.dot_general(a, b, (((1,), (1,)), ((), ())), preferred_element_type=F32)


def dot_nn(a, b):
    return lax.dot_general(a, b, (((1,), (0,)), ((), ())), preferred_element_type=F32)


def dot_tn(a, b):
    return lax.dot_general(a, b, (((0,), (0,)), ((), ())), preferred_element_type=F32)


def kernel(
    n,
    q_hbm, k_hbm, v_hbm, o_hbm, g_hbm, lse_hbm,
    gq_out, gk_out, gv_out,
    kin, kraw, kv_x, via_b, qraw, graw, ob, qf, gf, qt, gt, qx, gx, lse_s, st, stx, kf,
    acc_h, acc_l, dq_t, dqs, g2s, g2r, g1s, g1r, g0r, fi, fo,
    kv_ld, in_ld,
    o_send, o_recv, via_send, via_recv, r_send, r_recv, g2_send, g2_recv, g1_send, g1_recv,
    x_send, x_recv, dq_send, dq_recv, out_sem,
):
    me = lax.axis_index("seq")
    k = lax.rem(me, 2)
    oth = 1 - k
    chip = lax.div(me, 2)
    up = lax.rem(me - k + 2, n)
    down = lax.rem(me - k + n - 2, n)
    up3 = lax.rem(me - k + 6, n)
    down3 = lax.rem(me - k + n - 6, n)
    y = lax.rem(chip, 4)
    via_dev = jnp.where(y == 0, up3, down)
    onward = jnp.where(y == 3, down, up3)
    partner = me - k + oth

    def remote(src, dst, ssem, rsem, dev):
        return pltpu.make_async_remote_copy(
            src_ref=src, dst_ref=dst, send_sem=ssem, recv_sem=rsem,
            device_id=(dev,), device_id_type=MESH,
        )

    def par(u):
        return k if u % 2 == 0 else oth

    bar = pltpu.get_barrier_semaphore()
    for dev in (up, up + 1, down, down + 1, up3, up3 + 1, down3, down3 + 1, partner):
        pl.semaphore_signal(bar, inc=1, device_id=(dev,), device_id_type=MESH)

    kv_loads = []
    for m in range(NC):
        rows = pl.ds(m * TC, TC)
        for i, pair in enumerate((k, oth)):
            for e, src in enumerate((k_hbm, v_hbm)):
                kv_loads.append(
                    pltpu.make_async_copy(src.at[rows, pair], kin.at[i, m, e], kv_ld.at[m, i, e])
                )
    for m in (0, VIA, 1, 2):
        for c in kv_loads[4 * m : 4 * m + 4]:
            c.start()
    in_loads = []
    s = 0
    for src, dst2 in ((q_hbm, qraw), (g_hbm, graw), (o_hbm, ob)):
        for i, base in enumerate((k, oth)):
            for j in range(2):
                in_loads.append(
                    pltpu.make_async_copy(src.at[:, 2 * base + j], dst2.at[i, j], in_ld.at[s])
                )
                s += 1
    in_loads.append(pltpu.make_async_copy(lse_hbm, lse_s, in_ld.at[s]))
    for c in in_loads:
        c.start()

    def own_copy(u):
        m = u // 2
        src = kraw.at[4 + k, m] if u % 2 == 0 else kv_x.at[m]
        dev = up + par(u)
        return remote(src, kraw.at[2 + k, m], o_send.at[u], o_recv.at[k, m], dev)

    def own_arrival(u):
        m = u // 2
        x = par(u)
        return remote(kraw.at[2 + x, m], kraw.at[2 + x, m], o_send.at[u], o_recv.at[x, m], up)

    def via_copy(u):
        src = kraw.at[4 + k, VIA] if u % 2 == 0 else kv_x.at[VIA]
        return remote(src, via_b.at[k], via_send.at[u % 2], via_recv.at[k], via_dev + par(u))

    def via_onward(u):
        x = par(u)
        return remote(via_b.at[x], kraw.at[x, VIA], r_send.at[u], r_recv.at[x, VIA], onward + k)

    def via_arrival(u):
        x = par(u)
        return remote(via_b.at[x], via_b.at[x], via_send.at[u % 2], via_recv.at[x], via_dev)

    def relay_copy(u):
        m = u // 2
        x = par(u)
        return remote(kraw.at[2 + x, m], kraw.at[x, m], r_send.at[u], r_recv.at[x, m], up + k)

    def g2_copy(m, j):
        return remote(g2s.at[m, j], g2r.at[m, j], g2_send.at[m, j], g2_recv.at[m, j], down + k)

    def g1_copy(u):
        m = u // 2
        x = par(u)
        return remote(g1s.at[m, x], g1r.at[k, m], g1_send.at[u], g1_recv.at[k, m], down + x)

    def g1_arrival(u):
        m = u // 2
        p = par(u)
        return remote(g1s.at[m, p], g1r.at[p, m], g1_send.at[u], g1_recv.at[p, m], down)

    x_kv = remote(kv_x, kraw.at[4 + k], x_send.at[0], x_recv.at[0], partner)
    x_q = remote(qx, qf.at[k], x_send.at[1], x_recv.at[1], partner)
    x_g = remote(gx, gf.at[k], x_send.at[2], x_recv.at[2], partner)
    x_st = remote(stx, st.at[k], x_send.at[3], x_recv.at[3], partner)
    g0_copy = remote(acc_l.at[oth], g0r, x_send.at[4], x_recv.at[4], partner)

    def kv_wait(m, i):
        for e in range(2):
            kv_loads[(m * 2 + i) * 2 + e].wait()

    def flat(val):
        return val.reshape(val.shape[0] * 2, HD)

    def split(m, send=None):
        for i, dst in enumerate((kraw.at[4 + k, m], kv_x.at[m])):
            kv_wait(m, i)
            for e in range(2):
                kf[e] = flat(kin[i, m, e]).astype(F32)
                for j in range(2):
                    dst[e, j] = kf[e, pl.ds(j, TC, stride=2), :].astype(BF)
            if send is not None:
                send(2 * m + i).start()

    split(0)
    pl.semaphore_wait(bar, 9)
    own_copy(0).start()
    own_copy(1).start()
    split(VIA, via_copy)
    split(1)
    split(2)
    x_kv.start()
    def rows_of_queries():
        for raw, near, far, first, copy in ((qraw, qf, qx, 0, x_q), (graw, gf, gx, 4, x_g)):
            for j in range(2):
                in_loads[first + 2 + j].wait()
                far[j] = flat(raw[1, j])
            copy.start()
            for j in range(2):
                in_loads[first + j].wait()
                near[k, j] = flat(raw[0, j])

    def statistics():
        for i in range(8, 13):
            in_loads[i].wait()
        lse = lse_s[...] * LOG2E
        hi = lse.astype(BF)
        rest = lse - hi.astype(F32)
        mid = rest.astype(BF)
        low = (rest - mid.astype(F32)).astype(BF)
        parts = jnp.concatenate([hi.astype(F32), mid.astype(F32), low.astype(F32), jnp.zeros_like(lse)], 0).astype(BF)
        row = lax.broadcasted_iota(jnp.int32, (T, 2 * T), 0)
        col = lax.broadcasted_iota(jnp.int32, (T, 2 * T), 1)
        wide = []
        for e in range(2):
            place = jnp.where(col == 2 * row + e, 1.0, 0.0).astype(BF)
            r = dot_nn(parts, place)
            wide.append(r[0:8] + r[8:16] + r[16:24])
        lse_w = [wide[0][2 * i : 2 * i + 1] + wide[1][2 * i + 1 : 2 * i + 2] for i in range(4)]
        ones = jnp.ones((8, HD), BF)

        def delta_of(a, b):
            prod = a.astype(F32) * b.astype(F32)
            top = prod.astype(BF)
            left = (prod - top.astype(F32)).astype(BF)
            return (dot_nt(ones, top) + dot_nt(ones, left))[0:1]

        no_1 = jnp.where(chip < 1, FAR, 0.0).astype(F32)
        no_2 = jnp.where(chip < 2, FAR, 0.0).astype(F32)
        for j in range(2):
            for which in range(2):
                if which == 0:
                    dst, dl = st.at[k, j], delta_of(gf[k, j], flat(ob[0, j]))
                else:
                    dst, dl = stx.at[j], delta_of(gx[j], flat(ob[1, j]))
                if which == 0:
                    lw = jnp.where(k == 0, lse_w[j], lse_w[2 + j])
                else:
                    lw = jnp.where(k == 0, lse_w[2 + j], lse_w[j])
                dst[0:1, :] = lw
                dst[1:2, :] = dl
                dst[2:3, :] = lw + no_1
                dst[3:4, :] = lw + no_2
                dst[4:8, :] = jnp.zeros((4, 2 * T), F32)
        x_st.start()
        dq_t[...] = jnp.zeros_like(dq_t)

    def flip(b):
        for j in range(2):
            qt[b, j] = qf[b, j].T
            gt[b, j] = gf[b, j].T

    def tile(kc, vc, b, j, lo, norm_row, mask):
        q, g = qf[b, j, lo:, :], gf[b, j, lo:, :]
        sc = dot_nn(kc, qt[b, j, :, lo:])
        dp = dot_nn(vc, gt[b, j, :, lo:])
        p = jnp.exp2(sc * (SCALE * LOG2E) - st[b, j, norm_row : norm_row + 1, lo:])
        if mask is not None:
            p = jnp.where(mask, p, 0.0)
        dv = dot_nn(p.astype(BF), g)
        ds = (p * (dp - st[b, j, 1:2, lo:])).astype(BF)
        dk = dot_nn(ds, q)
        dq_t[b, j, :, lo:] += dot_tn(kc, ds)
        return dk, dv

    def keys(j, *parts):
        return [jnp.concatenate([kraw[x, m, e, j] for x, m in parts], 0) for e in range(2)]

    def heads(body):
        lax.fori_loop(0, 2, lambda j, c: (body(j), c)[1], 0)

    def grid2(rows, lo):
        row = lax.broadcasted_iota(jnp.int32, (rows, 2 * T - lo), 0)
        tok = (lo + lax.broadcasted_iota(jnp.int32, (rows, 2 * T - lo), 1)) // 2
        return row, tok

    R = 2 * TC

    def local_causal(x):
        for h in range(NC // 2):
            lo = 2 * h * R

            def body(j):
                row, tok = grid2(R, lo)
                kc, vc = keys(j, (4 + x, 2 * h), (4 + x, 2 * h + 1))
                dk, dv = tile(kc, vc, x, j, lo, 0, tok >= row + h * R)
                acc_l[x, 0, j, pl.ds(h * R, R), :] = dk
                acc_l[x, 1, j, pl.ds(h * R, R), :] = dv

            heads(body)

    def local_full():
        for h in range(NC // 2):

            def body(j):
                kc, vc = keys(j, (4, 2 * h), (4, 2 * h + 1))
                dk, dv = tile(kc, vc, 1, j, 0, 0, None)
                acc_l[0, 0, j, pl.ds(h * R, R), :] += dk
                acc_l[0, 1, j, pl.ds(h * R, R), :] += dv

            heads(body)

    def near(m):
        def body(j):
            kc, vc = keys(j, (2, m), (3, m))
            dk0, dv0 = tile(kc, vc, 0, j, 0, 2, None)
            dk1, dv1 = tile(kc, vc, 1, j, 0, 2, None)
            acc_h[m, 0, j] = dk0 + dk1
            acc_h[m, 1, j] = dv0 + dv1

        heads(body)

    def far(m):
        def body(j):
            row, tok = grid2(R, 0)
            kc, vc = keys(j, (0, m), (1, m))
            dk0, dv0 = tile(kc, vc, 0, j, 0, 3, (row >= TC) | (row + m * TC > tok))
            row, tok = grid2(TC, 0)
            dk1, dv1 = tile(kc[TC:], vc[TC:], 1, j, 0, 3, row + m * TC > tok)
            g2s[m, j, 0, 0] = dk0[:TC].astype(BF)
            g2s[m, j, 0, 1] = dv0[:TC].astype(BF)
            g2s[m, j, 1, 0] = (dk0[TC:] + dk1).astype(BF)
            g2s[m, j, 1, 1] = (dv0[TC:] + dv1).astype(BF)
            g2_copy(m, j).start()

        heads(body)

    def near_finish(m):
        for j in range(2):
            g2_copy(m, j).wait_recv()
            for x in range(2):
                for e in range(2):
                    val = acc_h[m, e, j, x * TC : (x + 1) * TC]
                    val = val + g2r[m, j, x, e].astype(F32)
                    g1s[m, x, e, j] = val.astype(BF)

    outs = []

    def final_unit(u):
        m, p = u // 2, par(u)
        rows = pl.ds(m * TC, TC)
        for e in range(2):
            for j in range(2):
                mine = acc_l[k, e, j, rows, :] if u % 2 == 0 else g0r[e, j, rows, :]
                val = mine + g1r[p, m, e, j].astype(F32)
                if e == 0:
                    val = val * SCALE
                fi[e, pl.ds(j, TC, stride=2), :] = val
            fo[u, e] = fi[e].astype(BF)
            dst = (gk_out, gv_out)[e]
            c = pltpu.make_async_copy(fo.at[u, e], dst.at[p, pl.ds(2 * m * TC, 2 * TC)], out_sem.at[2 * u + e])
            c.start()
            outs.append(c)

    def arrive(u):
        own_arrival(u).wait_recv()
        if u // 2 != VIA:
            relay_copy(u).start()
        if u + 2 < NU:
            own_copy(u + 2).start()

    def pass_on():
        for u in (2 * VIA, 2 * VIA + 1):
            via_arrival(u).wait_recv()
            via_onward(u).start()

    def far_step(m):
        relay_copy(2 * m).wait_recv()
        relay_copy(2 * m + 1).wait_recv()
        far(m)

    def near_step(m):
        near_finish(m)
        g1_copy(2 * m).start()
        g1_copy(2 * m + 1).start()

    def final_step(u):
        g1_arrival(u).wait_recv()
        final_unit(u)

    def from_partner():
        for c in (x_kv, x_q, x_g, x_st):
            c.wait_recv()

    def local_rest():
        local_full()
        g0_copy.start()

    dq_copies = []

    def query_grads():
        for j in range(2):
            for b in (oth, k):
                dqs[b, j] = (dq_t[b, j].T * SCALE).astype(BF)
            c = remote(dqs.at[oth, j], gq_out.at[2 * k + j], dq_send.at[j], dq_recv.at[j], partner)
            c.start()
            dq_copies.append(c)
            c = pltpu.make_async_copy(dqs.at[k, j], gq_out.at[2 * k + j], out_sem.at[2 * NU + j])
            c.start()
            outs.append(c)

    steps = {
        "flip0": lambda: flip(k), "flip1": lambda: flip(oth),
        "L0": lambda: local_causal(k), "L1": lambda: local_causal(oth), "LF": local_rest,
        "X": from_partner, "G": rows_of_queries, "T": statistics, "V": pass_on, "Q": lambda: g0_copy.wait_recv(), "D": query_grads,
    }
    by_index = {"A": arrive, "N": near, "F": far_step, "S": near_step, "Z": final_step}
    for word in PLAN:
        if word in steps:
            steps[word]()
        else:
            by_index[word[0]](int(word[1:]))

    for u in range(NU):
        own_copy(u).wait_send()
        (via_onward if u // 2 == VIA else relay_copy)(u).wait_send()
        if u // 2 == VIA:
            via_copy(u).wait_send()
        g1_copy(u).wait_send()
    for m in range(NC):
        for j in range(2):
            g2_copy(m, j).wait_send()
    for c in (x_kv, x_q, x_g, x_st, g0_copy):
        c.wait_send()
    for c in dq_copies:
        c.wait()
    for c in outs:
        c.wait()


def deliver(q_in, k_in, v_in, q_out, k_out, v_out, sem):
    copies = []
    for src, dst in ((q_in, q_out), (k_in, k_out), (v_in, v_out)):
        for p in range(src.shape[0]):
            copies.append(pltpu.make_async_copy(src.at[p], dst.at[:, p], sem.at[len(copies)]))
    for c in copies:
        c.start()
    for c in copies:
        c.wait()


def shards(n, queries, key_rows, value_rows, attn_output, grad_output, log_norm):
    heads4 = (T, 4, 2, HD)
    heads2 = (T, 2, 2, HD)
    anym = pl.BlockSpec(memory_space=pl.ANY)
    dma = pltpu.SemaphoreType.DMA
    vm = pltpu.VMEM
    pair = (T, 2, HD)
    scratch = [
        vm((2, NC, 2, TC, 2, HD), BF),
        vm((6, NC, 2, 2, TC, HD), BF),
        vm((NC, 2, 2, TC, HD), BF),
        vm((2, 2, 2, TC, HD), BF),
        vm((2, 2) + pair, BF),
        vm((2, 2) + pair, BF),
        vm((2, 2) + pair, BF),
        vm((2, 2, 2 * T, HD), BF),
        vm((2, 2, 2 * T, HD), BF),
        vm((2, 2, HD, 2 * T), BF),
        vm((2, 2, HD, 2 * T), BF),
        vm((2, 2 * T, HD), BF),
        vm((2, 2 * T, HD), BF),
        vm((8, T), F32),
        vm((2, 2, 8, 2 * T), F32),
        vm((2, 8, 2 * T), F32),
        vm((2, 2 * TC, HD), F32),
        vm((NC, 2, 2, 2 * TC, HD), F32),
        vm((2, 2, 2, T, HD), F32),
        vm((2, 2, HD, 2 * T), F32),
        vm((2, 2, 2 * T, HD), BF),
        vm((NC, 2, 2, 2, TC, HD), BF),
        vm((NC, 2, 2, 2, TC, HD), BF),
        vm((NC, 2, 2, 2, TC, HD), BF),
        vm((2, NC, 2, 2, TC, HD), BF),
        vm((2, 2, T, HD), F32),
        vm((2, 2 * TC, HD), F32),
        vm((NU, 2, 2 * TC, HD), BF),
        dma((NC, 2, 2)),
        dma((13,)),
        dma((NU,)), dma((2, NC)),
        dma((2,)), dma((2,)),
        dma((NU,)), dma((2, NC)),
        dma((NC, 2)), dma((NC, 2)),
        dma((NU,)), dma((2, NC)),
        dma((5,)), dma((5,)),
        dma((2,)), dma((2,)),
        dma((2 * NU + 2,)),
    ]
    gq, gk, gv = pl.pallas_call(
        functools.partial(kernel, n),
        out_shape=(
            jax.ShapeDtypeStruct((4, 2 * T, HD), BF),
            jax.ShapeDtypeStruct((2, 2 * T, HD), BF),
            jax.ShapeDtypeStruct((2, 2 * T, HD), BF),
        ),
        in_specs=[pl.BlockSpec(memory_space=pltpu.HBM)] * 6,
        out_specs=(anym,) * 3,
        scratch_shapes=scratch,
        compiler_params=pltpu.CompilerParams(
            collective_id=0, has_side_effects=True, vmem_limit_bytes=VMEM_KIB << 10
        ),
    )(
        *(
            pltpu.with_memory_space_constraint(a, pltpu.HBM)
            for a in (
                queries.reshape(heads4),
                key_rows.reshape(heads2),
                value_rows.reshape(heads2),
                attn_output.reshape(heads4),
                grad_output.reshape(heads4),
                log_norm,
            )
        )
    )
    gq, gk, gv = pl.pallas_call(
        deliver,
        out_shape=tuple(jax.ShapeDtypeStruct(shape, BF) for shape in (heads4, heads2, heads2)),
        in_specs=[anym] * 3,
        out_specs=(pl.BlockSpec(memory_space=pltpu.HBM),) * 3,
        scratch_shapes=[dma((8,))],
        compiler_params=pltpu.CompilerParams(vmem_limit_bytes=1 << 20),
    )(*(a.reshape((a.shape[0],) + pair) for a in (gq, gk, gv)))
    return (
        gq.reshape(queries.shape),
        gk.reshape(key_rows.shape),
        gv.reshape(value_rows.shape),
    )


def solution(mesh):
    wide = P("seq", None, None)
    return jax.shard_map(
        functools.partial(shards, mesh.shape["seq"]),
        mesh=mesh,
        in_specs=(wide, wide, wide, wide, wide, P(None, "seq")),
        out_specs=(wide, wide, wide),
        check_vma=False,
    )
```
